32 devices in a mesh: pb: 4 (over x, core), ka: 8 (over z, y).
Axes of the slice: x: 2, y: 2, z: 4, core: 2. Of those that a mesh axis runs over, the one named last changes fastest.
Arguments:
- queries: bfloat16 [4096, 1024], P(('pb', 'ka')), may hold values from -6 to 6
- key_rows: bfloat16 [4096, 128], P(('pb', 'ka')), may hold values from -6 to 6
- value_rows: bfloat16 [4096, 128], P(('pb', 'ka')), may hold values from -6 to 6
- forward_out: bfloat16 [4096, 1024], P(('pb', 'ka')), may hold values from -6 to 6
- out_grad: bfloat16 [4096, 1024], P(('pb', 'ka')), may hold values from -4 to 4
- logsumexp: float32 [8, 4096], P(None, ('pb', 'ka')), may hold values from 3 to 7
- position: int32 [4096], P(('pb', 'ka')), may hold values from 0 to 4095, as said below
- segment: int32 [4096], P(('pb', 'ka')), may hold values from 0 to 7, as said below
Outputs:
- query_grad: bfloat16 [4096, 1024], P(('pb', 'ka'))
- key_grad: bfloat16 [4096, 128], P(('pb', 'ka'))
- value_grad: bfloat16 [4096, 128], P(('pb', 'ka'))
The draws below stay inside these ranges and needn't reach their ends.
Inputs may be any that keep to these rules, and one draw needn't show every extreme that they name: `position`: a permutation of 0 to 4095; each aligned run of 128 rows holds 128 consecutive positions in increasing order. `segment`: the document of the row's position; each document is a nonempty run of consecutive positions, numbered in the order of positions, 8 documents in all.
All inputs are finite; a program needn't handle non-finite values.
Results may differ from the reference program's by a relative error of at most 0.0051.
Values may be sent and summed in bfloat16 or wider, within the bound.
A program may use at most 64 MiB of HBM per device.

```python
import jax
import jax.numpy as jnp
from jax import lax

HEADS = 8
HD = 128
TOK_DEV = 128
DOCS = 8
LENGTH = 4096


def build_layout(key):
    perm_key = jax.random.fold_in(key, 11)
    doc_key = jax.random.fold_in(key, 12)
    block_total = LENGTH // TOK_DEV
    block_order = jax.random.permutation(perm_key, block_total).astype(jnp.int32)
    position = (block_order[:, None] * TOK_DEV + jnp.arange(TOK_DEV, dtype=jnp.int32)[None, :]).reshape(-1).astype(jnp.int32)
    boundaries = (jax.random.choice(doc_key, LENGTH - 1, (DOCS - 1,), replace=False) + 1).astype(jnp.int32)
    document_ids = jnp.sum((jnp.arange(LENGTH, dtype=jnp.int32)[:, None] >= boundaries[None, :]).astype(jnp.int32), axis=1).astype(jnp.int32)
    segment = document_ids[position].astype(jnp.int32)
    return (position, segment)


def draw_position(key, part):
    return build_layout(key)[0]


def draw_segment(key, part):
    return build_layout(key)[1]


def level_of(own_key, dims, shards, least, largest):
    level, own = 1.0, jax.random.fold_in(own_key, 6)
    for dim, blocks in shards:
        steps = jnp.exp(jax.random.uniform(jax.random.fold_in(own, dim), (blocks,), jnp.float32, least / len(shards), largest / len(shards)))
        level = level * jnp.repeat(steps, dims[dim] // blocks).reshape([-1 if axis == dim else 1 for axis in range(len(dims))])
    return level


def centred(stream_key, extent, spread, reach, pieces=(), kind=jnp.bfloat16):
    entries = spread * jax.random.normal(stream_key, extent, jnp.float32)
    if pieces:
        entries = entries * level_of(stream_key, extent, pieces, -0.22, 0.18)
    return jnp.clip(entries, -reach, reach).astype(kind)


def setup_inputs(seed: int = 0) -> dict:
    seeds = jax.random.split(jax.random.key(seed), 9)
    return {
        "queries": centred(seeds[0], (LENGTH, HEADS * HD), 1.0, 6.0, ((0, 32),)),
        "key_rows": centred(seeds[1], (LENGTH, HD), 1.0, 6.0, ((0, 32),)),
        "value_rows": centred(seeds[2], (LENGTH, HD), 1.0, 6.0, ((0, 32),)),
        "forward_out": centred(seeds[3], (LENGTH, HEADS * HD), 0.5, 6.0, ((0, 32),)),
        "out_grad": centred(seeds[4], (LENGTH, HEADS * HD), 0.25, 4.0, ((0, 32),)),
        "logsumexp": jnp.clip(3.0 + 4.0 * jax.random.uniform(seeds[5], (HEADS, LENGTH), jnp.float32) ** level_of(seeds[5], (HEADS, LENGTH), ((1, 32),), -0.2, 0.2), 3.0, 7.0),
        "position": draw_position(jax.random.fold_in(seeds[8], 71), 0),
        "segment": draw_segment(jax.random.fold_in(seeds[8], 71), 0),
    }


def reference(queries, key_rows, value_rows, forward_out, out_grad, logsumexp, position, segment):
    head_width = key_rows.shape[1]
    row_count = queries.shape[0]
    head_count = queries.shape[1] // head_width
    score_scale = head_width ** -0.5
    highest = lax.Precision.HIGHEST
    delta_rows = jnp.sum((out_grad.astype(jnp.float32) * forward_out.astype(jnp.float32)).reshape(row_count, head_count, head_width), axis=2).T
    block_rows = min(512, row_count)
    block_count = row_count // block_rows
    key_float = key_rows.astype(jnp.float32)
    value_float = value_rows.astype(jnp.float32)

    def scan_step(loop_state, block_index):
        key_acc, value_acc = loop_state
        first_row = (block_index * block_rows).astype(jnp.int32)
        query_tile = lax.dynamic_slice_in_dim(queries, first_row, block_rows, 0).astype(jnp.float32).reshape(block_rows, head_count, head_width)
        grad_tile = lax.dynamic_slice_in_dim(out_grad, first_row, block_rows, 0).astype(jnp.float32).reshape(block_rows, head_count, head_width)
        lse_tile = lax.dynamic_slice_in_dim(logsumexp, first_row, block_rows, 1)
        delta_tile = lax.dynamic_slice_in_dim(delta_rows, first_row, block_rows, 1)
        place_tile = lax.dynamic_slice_in_dim(position, first_row, block_rows, 0)
        doc_tile = lax.dynamic_slice_in_dim(segment, first_row, block_rows, 0)
        visible = (position[None, :] <= place_tile[:, None]) & (segment[None, :] == doc_tile[:, None])
        scores = jnp.einsum("qhd,kd->hqk", query_tile, key_float, precision=highest) * score_scale
        weights = jnp.where(visible[None], jnp.exp(scores - lse_tile[:, :, None]), 0.0)
        rounded = lax.optimization_barrier(weights.astype(jnp.bfloat16)).astype(jnp.float32)
        value_acc = value_acc + jnp.einsum("hqk,qhd->kd", rounded, grad_tile, precision=highest)
        grad_scores = jnp.einsum("qhd,kd->hqk", grad_tile, value_float, precision=highest)
        score_grads = lax.optimization_barrier((weights * (grad_scores - delta_tile[:, :, None])).astype(jnp.bfloat16)).astype(jnp.float32)
        query_part = jnp.einsum("hqk,kd->qhd", score_grads, key_float, precision=highest).reshape(block_rows, head_count * head_width) * score_scale
        key_acc = key_acc + jnp.einsum("hqk,qhd->kd", score_grads, query_tile, precision=highest)
        return (key_acc, value_acc), query_part.astype(jnp.bfloat16)

    starting = (jnp.zeros((row_count, head_width), jnp.float32), jnp.zeros((row_count, head_width), jnp.float32))
    (key_acc, value_acc), grad_blocks = lax.scan(scan_step, starting, jnp.arange(block_count, dtype=jnp.int32))
    query_grad = grad_blocks.reshape(row_count, head_count * head_width)
    return query_grad, (key_acc * score_scale).astype(jnp.bfloat16), value_acc.astype(jnp.bfloat16)
```

```python
import functools

import jax
import jax.numpy as jnp
from jax import lax
from jax.experimental import pallas as pl
from jax.experimental.pallas import tpu as pltpu
from jax.sharding import PartitionSpec as P

MESH = pl.DeviceIdType.MESH
LOG2E = 1.4426950408889634
HIDDEN = -1e30
NT = (((1,), (1,)), ((), ()))
F32 = jnp.float32
BF16 = jnp.bfloat16


def schedule(nz):
    late = (0.0, 1.3, 1.4, 2.6)
    order = sorted((dz + late[dp], dz, dp) for dz in range(nz) for dp in range(4))
    blocks = [b[1:] for b in order]
    steps = [blocks[i:i + 2] for i in range(0, len(blocks), 2)]
    when = {b: t for t, step in enumerate(steps) for b in step}
    folded = list(range(1, nz // 2))
    return steps, when, list(range(nz // 2, nz)), folded


def kernel(
    pb_size, ka_size,
    q_hbm, g_hbm, o_hbm, k_hbm, v_hbm, lse_ref, place_ref, doc_ref,
    dq_ref, dk_ref, dv_ref,
    kv, qs, gs, os, own, sp, bias, pt, st, dqt, dqr,
    part, red, acc, zpart, zred, fold,
    load, kv_send, kv_recv, relay_send, relay_recv, pair_send, pair_recv,
    red_send, red_recv, z_send, z_recv, fold_send, fold_recv,
):
    rows, width = dk_ref.shape
    heads = q_hbm.shape[1] // width
    both = 2 * rows
    scale = width ** (-0.5)
    nz, plane = ka_size // 2, pb_size
    pb, ka = lax.axis_index("pb"), lax.axis_index("ka")
    hi, core = pb // 2, lax.rem(pb, 2)
    z, low = ka // 2, lax.rem(ka, 2)

    def place(dz, dp):
        up, bit = z, 1
        while bit < nz:
            mine, flip = (z // bit) % 2, (dz // bit) % 2
            up = up + flip * (1 - 2 * mine) * bit
            bit *= 2
        far = 1 - hi if dp // 2 else hi
        near = 1 - low if dp % 2 else low
        return {"pb": far * 2 + core, "ka": up * 2 + near}

    partner = {"pb": hi * 2 + 1 - core, "ka": ka}

    def remote(src, dst, send, recv, device):
        return pltpu.make_async_remote_copy(
            src_ref=src, dst_ref=dst, send_sem=send, recv_sem=recv,
            device_id=device, device_id_type=MESH,
        )

    loads = [
        pltpu.make_async_copy(k_hbm, kv.at[0, 0, pl.ds(0, rows)], load.at[0]),
        pltpu.make_async_copy(v_hbm, kv.at[0, 0, pl.ds(rows, rows)], load.at[1]),
    ]
    for src, dst in ((q_hbm, qs), (g_hbm, gs), (o_hbm, os)):
        for h in range(heads):
            loads.append(pltpu.make_async_copy(
                src.at[:, pl.ds(h * width, width)], dst.at[h, pl.ds(0, rows)], load.at[len(loads)]
            ))
    for copy in loads:
        copy.start()

    barrier = pltpu.get_barrier_semaphore()
    steps, when, direct, folded = schedule(nz)
    last = len(steps) - 1
    peers = [place(dz, 0) for dz in range(1, nz)] + [place(0, dp) for dp in range(1, plane)] + [partner]
    peers += [place(dz, 3) for dz in direct]
    for peer in peers:
        pl.semaphore_signal(barrier, inc=1, device_id=peer, device_id_type=MESH)

    spots = place_ref[...].astype(F32)
    docs = doc_ref[...].astype(F32)
    line = lax.broadcasted_iota(jnp.int32, (16, rows), 0)
    first = jnp.min(spots, axis=1, keepdims=True) * (1.0 / rows)
    meta = jnp.where(line == 0, jnp.broadcast_to(first, (16, rows)), jnp.broadcast_to(docs, (16, rows)))
    kv[0, 0, both:both + 16, :] = meta.astype(BF16)
    own[:heads] = lse_ref[...]
    own[2 * heads:2 * heads + 8] = jnp.where(
        line[:8] == 0, jnp.broadcast_to(spots, (8, rows)), jnp.broadcast_to(docs, (8, rows))
    )
    for copy in loads[:2]:
        copy.wait()
    pl.semaphore_wait(barrier, len(peers))

    def column_copy(dz):
        return remote(kv.at[0, 0], kv.at[dz, 0], kv_send.at[dz, 0], kv_recv.at[dz, 0], place(dz, 0))

    def plane_copy(dz, dp):
        return remote(kv.at[dz, 0], kv.at[dz, dp], kv_send.at[dz, dp], kv_recv.at[dz, dp], place(0, dp))

    def relay_copy(dz, dp):
        piece = pl.ds(0, rows) if dp == 1 else pl.ds(rows, rows + 16)
        return remote(
            kv.at[dz, 3 - dp, piece], kv.at[dz, 3, piece],
            relay_send.at[dz, dp - 1], relay_recv.at[dz, dp - 1], place(0, dp),
        )

    def part_copy(dz, dp):
        far = dz if dp == 3 and dz in direct else 0
        return remote(part.at[dz, dp], red.at[dz, dp], red_send.at[dz, dp], red_recv.at[dz, dp], place(far, dp))

    def fold_copy(dz):
        return remote(part.at[dz, 3], fold.at[dz], fold_send.at[dz], fold_recv.at[dz], place(dz, 0))

    def z_copy(dz):
        return remote(zpart.at[dz], zred.at[dz], z_send.at[dz], z_recv.at[dz], place(dz, 0))

    ours, theirs = pl.ds(0, rows), pl.ds(rows, rows)
    pair = [
        remote(src, dst, pair_send.at[i], pair_recv.at[i], partner)
        for i, (src, dst) in enumerate((
            (qs.at[:, ours], qs.at[:, theirs]), (gs.at[:, ours], gs.at[:, theirs]),
            (own, sp), (dqt.at[1], dqr),
        ))
    ]
    for dp in (1, 2):
        plane_copy(0, dp).start()
    for dz in range(1, nz):
        column_copy(dz).start()
    plane_copy(0, 3).start()
    dqt[...] = jnp.zeros_like(dqt)
    for copy in loads[2:2 + 2 * heads]:
        copy.wait()
    for copy in pair[:2]:
        copy.start()
    for copy in loads[2 + 2 * heads:]:
        copy.wait()
    for h in range(heads):
        product = gs[h, :rows].astype(F32) * os[h].astype(F32)
        own[heads + h:heads + h + 1] = jnp.sum(product.T, axis=0, keepdims=True)
    pair[2].start()

    def spread(dz):
        column_copy(dz).wait_recv()
        for dp in (1, 2):
            plane_copy(dz, dp).start()

    def pass_on(dz):
        for dp in (2, 1):
            plane_copy(dz, 3 - dp).wait_recv()
            relay_copy(dz, dp).start()

    for copy in pair[:3]:
        copy.wait_recv()

    def stat_row(i):
        return jnp.concatenate([own[i:i + 1, :], sp[i:i + 1, :]], axis=1)

    place_q = stat_row(2 * heads)
    doc_q = stat_row(2 * heads + 1)

    def key_side(dz, dp):
        meta = kv[dz, dp, both:both + 16, :].astype(F32)
        base = jnp.broadcast_to(meta[0:1, :], (rows, rows))
        doc = jnp.broadcast_to(meta[1:2, :], (rows, rows)).T
        spot = base * float(rows) + lax.broadcasted_iota(jnp.int32, (rows, rows), 0).astype(F32)
        return spot, doc

    def step(blocks):
        (za, pa), (zb, pc) = blocks
        for i, (dz, dp) in enumerate(blocks):
            spot, doc = key_side(dz, dp)
            for c in range(2):
                lanes = slice(c * rows, (c + 1) * rows)
                seen = (spot <= place_q[:, lanes]) & (doc == doc_q[:, lanes])
                bias[i * rows:(i + 1) * rows, lanes] = jnp.where(seen, 0.0, HIDDEN)
        kb = jnp.concatenate([kv[za, pa, :rows, :], kv[zb, pc, :rows, :]], axis=0)
        vb = jnp.concatenate([kv[za, pa, rows:both, :], kv[zb, pc, rows:both, :]], axis=0)
        kt = kb.T
        for h in range(heads):
            s = lax.dot_general(kb, qs[h], NT, preferred_element_type=F32)
            d = lax.dot_general(vb, gs[h], NT, preferred_element_type=F32)
            w = jnp.exp2(s * (scale * LOG2E) + (bias[...] - stat_row(h) * LOG2E))
            pt[:, h * both:(h + 1) * both] = w.astype(BF16)
            st[:, h * both:(h + 1) * both] = (w * (d - stat_row(heads + h))).astype(BF16)
        dv = jnp.dot(pt[...], gs[...].reshape(heads * both, width), preferred_element_type=F32)
        dk = jnp.dot(st[...], qs[...].reshape(heads * both, width), preferred_element_type=F32)
        for i, (dz, dp) in enumerate(blocks):
            piece = slice(i * rows, (i + 1) * rows)
            acc[dz, dp, :rows] = dk[piece]
            acc[dz, dp, rows:] = dv[piece]
            part[dz, dp, :rows] = dk[piece].astype(BF16)
            part[dz, dp, rows:] = dv[piece].astype(BF16)
        for h in range(heads):
            dq = jnp.dot(kt, st[:, h * both:(h + 1) * both], preferred_element_type=F32)
            dqt[0, h] += dq[:, :rows]
            dqt[1, h] += dq[:, rows:]

    def plane_sum(dz):
        total = acc[dz, 0]
        for dp in (1, 2):
            part_copy(dz, dp).wait_recv()
            total = total + red[dz, dp].astype(F32)
        return total

    def send_sum(dz):
        zpart[dz] = plane_sum(dz).astype(BF16)
        z_copy(dz).start()

    def corner():
        total = acc[0, 3]
        for dz in folded:
            fold_copy(dz).wait_recv()
            total = total + fold[dz].astype(F32)
        part[0, 3] = total.astype(BF16)
        part_copy(0, 3).start()

    def before(t):
        for dz in range(1, nz):
            if max(0, when[dz, 0] - 1) == t:
                spread(dz)
        for b in steps[t]:
            if b[0] == 0 and b[1] > 0:
                plane_copy(*b).wait_recv()
        for dz in range(1, nz):
            if min(when[dz, 1], when[dz, 2]) == t:
                pass_on(dz)
        for b in steps[t]:
            if b[0] > 0 and b[1] == 3:
                for dp in (1, 2):
                    relay_copy(b[0], dp).wait_recv()

    def after(t):
        for dz, dp in steps[t]:
            if dp == 3 and dz in folded:
                fold_copy(dz).start()
            elif dp and (dz or dp < 3):
                part_copy(dz, dp).start()
        for dz in range(1, nz):
            if max(when[dz, 0], when[dz, 1], when[dz, 2]) + 2 == t:
                send_sum(dz)

    def pick(t, table):
        value = jnp.int32(table[-1])
        for k in range(len(table) - 1):
            value = jnp.where(t == k, table[k], value)
        return value

    def turn(t, carry):
        for k in range(len(steps)):
            pl.when(t == k)(functools.partial(before, k))
        step([[pick(t, [s[i][j] for s in steps]) for j in range(2)] for i in range(2)])
        for k in range(len(steps)):
            pl.when(t == k)(functools.partial(after, k))
        return carry

    lax.fori_loop(0, len(steps), turn, 0)
    pair[3].start()
    for dz in range(1, nz):
        if max(when[dz, 0], when[dz, 1], when[dz, 2]) + 2 > last:
            send_sum(dz)
    corner()
    pair[3].wait_recv()
    for h in range(heads):
        dq = (dqt[0, h] + dqr[h]) * scale
        dq_ref[:, h * width:(h + 1) * width] = dq.T.astype(BF16)
    total = plane_sum(0)
    part_copy(0, 3).wait_recv()
    total = total + red[0, 3].astype(F32)
    for dz in direct:
        part_copy(dz, 3).wait_recv()
        total = total + red[dz, 3].astype(F32)
    for dz in range(1, nz):
        z_copy(dz).wait_recv()
        total = total + zred[dz].astype(F32)
    dk_ref[...] = (total[:rows] * scale).astype(BF16)
    dv_ref[...] = total[rows:].astype(BF16)

    for copy in pair:
        copy.wait_send()
    for dz in range(nz):
        for dp in (1, 2):
            part_copy(dz, dp).wait_send()
            plane_copy(dz, dp).wait_send()
            if dz > 0:
                relay_copy(dz, dp).wait_send()
        if dz in folded:
            fold_copy(dz).wait_send()
        else:
            part_copy(dz, 3).wait_send()
        if dz > 0:
            column_copy(dz).wait_send()
            z_copy(dz).wait_send()
    plane_copy(0, 3).wait_send()


def write_out(*refs):
    for src, dst in zip(refs[:3], refs[3:]):
        dst[...] = src[...]


def solution(mesh):
    pb_size, ka_size = mesh.shape["pb"], mesh.shape["ka"]

    def body(queries, key_rows, value_rows, forward_out, out_grad, logsumexp, position, segment):
        rows, width = key_rows.shape
        heads = queries.shape[1] // width
        nz, plane = ka_size // 2, pb_size
        both = 2 * rows
        dma, vmem = pltpu.SemaphoreType.DMA, pltpu.VMEM
        space = pl.BlockSpec(memory_space=pltpu.VMEM)
        grads = pl.pallas_call(
            functools.partial(kernel, pb_size, ka_size),
            out_shape=(
                jax.ShapeDtypeStruct(queries.shape, BF16),
                jax.ShapeDtypeStruct(key_rows.shape, BF16),
                jax.ShapeDtypeStruct(key_rows.shape, BF16),
            ),
            in_specs=[pl.BlockSpec(memory_space=pltpu.HBM)] * 5 + [space] * 3,
            out_specs=(space,) * 3,
            scratch_shapes=[
                vmem((nz, plane, both + 16, width), BF16),
                vmem((heads, both, width), BF16),
                vmem((heads, both, width), BF16),
                vmem((heads, rows, width), BF16),
                vmem((2 * heads + 8, rows), F32),
                vmem((2 * heads + 8, rows), F32),
                vmem((both, both), F32),
                vmem((both, heads * both), BF16),
                vmem((both, heads * both), BF16),
                vmem((2, heads, width, rows), F32),
                vmem((heads, width, rows), F32),
                vmem((nz, plane, both, width), BF16),
                vmem((nz, plane, both, width), BF16),
                vmem((nz, plane, both, width), F32),
                vmem((nz, both, width), BF16),
                vmem((nz, both, width), BF16),
                vmem((nz, both, width), BF16),
                dma((3 * heads + 2,)), dma((nz, plane)), dma((nz, plane)),
                dma((nz, 2)), dma((nz, 2)), dma((4,)), dma((4,)),
                dma((nz, plane)), dma((nz, plane)),
                dma((nz,)), dma((nz,)), dma((nz,)), dma((nz,)),
            ],
            compiler_params=pltpu.CompilerParams(
                collective_id=0, has_side_effects=True, vmem_limit_bytes=48 * 2**20
            ),
        )(*(pltpu.with_memory_space_constraint(x, pltpu.HBM) for x in (
            queries, out_grad, forward_out, key_rows, value_rows, logsumexp,
            position.reshape(1, rows), segment.reshape(1, rows),
        )))
        return pl.pallas_call(
            write_out,
            out_shape=tuple(jax.ShapeDtypeStruct(g.shape, g.dtype) for g in grads),
            in_specs=[space] * 3,
            out_specs=(space,) * 3,
            compiler_params=pltpu.CompilerParams(vmem_limit_bytes=4 * 2**20),
        )(*grads)

    flat = P(("pb", "ka"), None)
    line = P(("pb", "ka"))
    return jax.shard_map(
        body,
        mesh=mesh,
        in_specs=(flat,) * 5 + (P(None, ("pb", "ka")), line, line),
        out_specs=(flat,) * 3,
        check_vma=False,
    )
```

```python
import functools

import jax
import jax.numpy as jnp
from jax import lax
from jax.experimental import pallas as pl
from jax.experimental.pallas import tpu as pltpu
from jax.sharding import PartitionSpec as P

MESH = pl.DeviceIdType.MESH
LOG2E = 1.4426950408889634
HIDDEN = -1e30
NT = (((1,), (1,)), ((), ()))
F32 = jnp.float32
BF16 = jnp.bfloat16


def schedule(nz):
    ranks = [0, nz - 1] + list(range(1, nz - 1))
    order = []
    for r, dz in enumerate(ranks):
        late = (0.0, 0.5, 0.6, 1.1) if r == 0 else (0.0, 1.3, 1.4, {1: 2.65, 2: 1.45}.get(r, 1.5))
        order += [(r + late[dp], dz, dp) for dp in range(4)]
    order.sort()
    blocks = [b[1:] for b in order]
    steps = [blocks[i:i + 2] for i in range(0, len(blocks), 2)]
    when = {b: t for t, step in enumerate(steps) for b in step}
    part = max(1, nz // 4)
    climb = list(range(1, nz - 1))
    direct = ranks[-part:]
    folded = [dz for dz in range(1, part + 1) if dz not in direct]
    return steps, when, climb, direct, folded, ranks


def kernel(
    pb_size, ka_size,
    q_hbm, g_hbm, o_hbm, k_hbm, v_hbm, lse_ref, place_ref, doc_ref,
    dq_ref, dk_ref, dv_ref,
    kv, qs, gs, os, own, sp, bias, pt, st, dqt, dqr,
    part, red, acc, zpart, zred, fold,
    load, kv_send, kv_recv, relay_send, relay_recv, pair_send, pair_recv,
    red_send, red_recv, z_send, z_recv, fold_send, fold_recv,
):
    rows, width = dk_ref.shape
    heads = q_hbm.shape[1] // width
    both = 2 * rows
    scale = width ** (-0.5)
    nz, plane = ka_size // 2, pb_size
    pb, ka = lax.axis_index("pb"), lax.axis_index("ka")
    hi, core = pb // 2, lax.rem(pb, 2)
    z, low = ka // 2, lax.rem(ka, 2)

    def place(dz, dp):
        up, bit = z, 1
        while bit < nz:
            mine, flip = (z // bit) % 2, (dz // bit) % 2
            up = up + flip * (1 - 2 * mine) * bit
            bit *= 2
        far = 1 - hi if dp // 2 else hi
        near = 1 - low if dp % 2 else low
        return {"pb": far * 2 + core, "ka": up * 2 + near}

    partner = {"pb": hi * 2 + 1 - core, "ka": ka}

    def remote(src, dst, send, recv, device):
        return pltpu.make_async_remote_copy(
            src_ref=src, dst_ref=dst, send_sem=send, recv_sem=recv,
            device_id=device, device_id_type=MESH,
        )

    loads = [
        pltpu.make_async_copy(k_hbm, kv.at[0, 0, pl.ds(0, rows)], load.at[0]),
        pltpu.make_async_copy(v_hbm, kv.at[0, 0, pl.ds(rows, rows)], load.at[1]),
    ]
    for src, dst in ((q_hbm, qs), (g_hbm, gs), (o_hbm, os)):
        for h in range(heads):
            loads.append(pltpu.make_async_copy(
                src.at[:, pl.ds(h * width, width)], dst.at[h, pl.ds(0, rows)], load.at[len(loads)]
            ))
    for copy in loads:
        copy.start()

    barrier = pltpu.get_barrier_semaphore()
    steps, when, climb, direct, folded, ranks = schedule(nz)
    last = len(steps) - 1
    peers = [place(dz, 0) for dz in range(1, nz)] + [place(0, dp) for dp in range(1, plane)] + [partner]
    for peer in peers:
        pl.semaphore_signal(barrier, inc=1, device_id=peer, device_id_type=MESH)

    spots = place_ref[...].astype(F32)
    docs = doc_ref[...].astype(F32)
    line = lax.broadcasted_iota(jnp.int32, (16, rows), 0)
    first = jnp.min(spots, axis=1, keepdims=True) * (1.0 / rows)
    meta = jnp.where(line == 0, jnp.broadcast_to(first, (16, rows)), jnp.broadcast_to(docs, (16, rows)))
    kv[0, 0, both:both + 16, :] = meta.astype(BF16)
    own[:heads] = lse_ref[...]
    own[2 * heads:2 * heads + 8] = jnp.where(
        line[:8] == 0, jnp.broadcast_to(spots, (8, rows)), jnp.broadcast_to(docs, (8, rows))
    )
    for copy in loads[:2]:
        copy.wait()
    pl.semaphore_wait(barrier, len(peers))

    def column_copy(dz):
        return remote(kv.at[0, 0], kv.at[dz, 0], kv_send.at[dz, 0], kv_recv.at[dz, 0], place(dz, 0))

    def plane_copy(dz, dp):
        return remote(kv.at[dz, 0], kv.at[dz, dp], kv_send.at[dz, dp], kv_recv.at[dz, dp], place(0, dp))

    def relay_copy(dz, dp):
        piece = pl.ds(0, rows) if dp == 1 else pl.ds(rows, rows + 16)
        return remote(
            kv.at[dz, 3 - dp, piece], kv.at[dz, 3, piece],
            relay_send.at[dz, dp - 1], relay_recv.at[dz, dp - 1], place(0, dp),
        )

    def climb_copy(dz):
        return remote(kv.at[0, 3], kv.at[dz, 3], kv_send.at[dz, 3], kv_recv.at[dz, 3], place(dz, 0))

    def part_copy(dz, dp):
        far = dz if dp == 3 and dz in direct else 0
        return remote(part.at[dz, dp], red.at[dz, dp], red_send.at[dz, dp], red_recv.at[dz, dp], place(far, dp))

    def fold_copy(dz, dp):
        return remote(part.at[dz, dp], fold.at[dz, dp], fold_send.at[dz, dp], fold_recv.at[dz, dp], place(dz, 0))

    def z_copy(dz):
        return remote(zpart.at[dz], zred.at[dz], z_send.at[dz], z_recv.at[dz], place(dz, 0))

    ours, theirs = pl.ds(0, rows), pl.ds(rows, rows)
    pair = [
        remote(src, dst, pair_send.at[i], pair_recv.at[i], partner)
        for i, (src, dst) in enumerate((
            (qs.at[:, ours], qs.at[:, theirs]), (gs.at[:, ours], gs.at[:, theirs]),
            (own, sp), (dqt.at[1], dqr),
        ))
    ]
    for dp in (1, 2):
        plane_copy(0, dp).start()
    for dz in ranks[1:]:
        column_copy(dz).start()
    plane_copy(0, 3).start()
    dqt[...] = jnp.zeros_like(dqt)
    for copy in loads[2:2 + 2 * heads]:
        copy.wait()
    for copy in pair[:2]:
        copy.start()
    for copy in loads[2 + 2 * heads:]:
        copy.wait()
    for h in range(heads):
        product = gs[h, :rows].astype(F32) * os[h].astype(F32)
        own[heads + h:heads + h + 1] = jnp.sum(product.T, axis=0, keepdims=True)
    pair[2].start()

    def spread(dz):
        column_copy(dz).wait_recv()
        for dp in (1, 2):
            plane_copy(dz, dp).start()

    def pass_on(dz):
        for dp in (2, 1):
            plane_copy(dz, 3 - dp).wait_recv()
            if dz not in climb:
                relay_copy(dz, dp).start()

    for copy in pair[:3]:
        copy.wait_recv()

    def stat_row(i):
        return jnp.concatenate([own[i:i + 1, :], sp[i:i + 1, :]], axis=1)

    place_q = stat_row(2 * heads)
    doc_q = stat_row(2 * heads + 1)

    def key_side(dz, dp):
        meta = kv[dz, dp, both:both + 16, :].astype(F32)
        base = jnp.broadcast_to(meta[0:1, :], (rows, rows))
        doc = jnp.broadcast_to(meta[1:2, :], (rows, rows)).T
        spot = base * float(rows) + lax.broadcasted_iota(jnp.int32, (rows, rows), 0).astype(F32)
        return spot, doc

    def step(blocks):
        (za, pa), (zb, pc) = blocks
        for i, (dz, dp) in enumerate(blocks):
            spot, doc = key_side(dz, dp)
            for c in range(2):
                lanes = slice(c * rows, (c + 1) * rows)
                seen = (spot <= place_q[:, lanes]) & (doc == doc_q[:, lanes])
                bias[i * rows:(i + 1) * rows, lanes] = jnp.where(seen, 0.0, HIDDEN)
        kb = jnp.concatenate([kv[za, pa, :rows, :], kv[zb, pc, :rows, :]], axis=0)
        vb = jnp.concatenate([kv[za, pa, rows:both, :], kv[zb, pc, rows:both, :]], axis=0)
        kt = kb.T
        for h in range(heads):
            s = lax.dot_general(kb, qs[h], NT, preferred_element_type=F32)
            d = lax.dot_general(vb, gs[h], NT, preferred_element_type=F32)
            w = jnp.exp2(s * (scale * LOG2E) + (bias[...] - stat_row(h) * LOG2E))
            pt[:, h * both:(h + 1) * both] = w.astype(BF16)
            st[:, h * both:(h + 1) * both] = (w * (d - stat_row(heads + h))).astype(BF16)
        dv = jnp.dot(pt[...], gs[...].reshape(heads * both, width), preferred_element_type=F32)
        dk = jnp.dot(st[...], qs[...].reshape(heads * both, width), preferred_element_type=F32)
        for i, (dz, dp) in enumerate(blocks):
            piece = slice(i * rows, (i + 1) * rows)
            acc[dz, dp, :rows] = dk[piece]
            acc[dz, dp, rows:] = dv[piece]
            part[dz, dp, :rows] = dk[piece].astype(BF16)
            part[dz, dp, rows:] = dv[piece].astype(BF16)
        for h in range(heads):
            dq = jnp.dot(kt, st[:, h * both:(h + 1) * both], preferred_element_type=F32)
            dqt[0, h] += dq[:, :rows]
            dqt[1, h] += dq[:, rows:]

    def plane_sum(dz):
        total = acc[dz, 0]
        for dp in () if dz in folded else (1, 2) if dz == 0 or dz in direct else (1, 2, 3):
            part_copy(dz, dp).wait_recv()
            total = total + red[dz, dp].astype(F32)
        return total

    def send_sum(dz):
        zpart[dz] = plane_sum(dz).astype(BF16)
        z_copy(dz).start()

    def merge(dp):
        total = acc[0, dp]
        for dz in folded:
            fold_copy(dz, dp).wait_recv()
            total = total + fold[dz, dp].astype(F32)
        part[0, dp] = total.astype(BF16)
        part_copy(0, dp).start()

    def before(t):
        if t == when[0, 3]:
            plane_copy(0, 3).wait_recv()
            for dz in climb:
                climb_copy(dz).start()
        for r, dz in enumerate(ranks):
            if r and max(0, when[dz, 0] - {1: 0, 2: 0}.get(r, 1)) == t:
                spread(dz)
        for b in steps[t]:
            if b[0] == 0 and b[1] in (1, 2):
                plane_copy(*b).wait_recv()
        for dz in ranks[1:]:
            if min(when[dz, 1], when[dz, 2]) == t:
                pass_on(dz)
        for b in steps[t]:
            if b[0] in climb and b[1] == 3:
                climb_copy(b[0]).wait_recv()
            elif b[0] > 0 and b[1] == 3:
                for dp in (1, 2):
                    relay_copy(b[0], dp).wait_recv()

    def after(t):
        for dz, dp in steps[t]:
            if dp and dz in folded:
                fold_copy(dz, dp).start()
            elif dp and dz:
                part_copy(dz, dp).start()
        if t == last:
            for dp in (3, 1, 2):
                merge(dp)
        for dz in ranks[1:]:
            ready = when[dz, 0] if dz in folded else max(when[dz, dp] for dp in range(3 if dz in direct else 4)) + 2
            if min(ready, last) == t:
                send_sum(dz)

    def pick(t, table):
        value = jnp.int32(table[-1])
        for k in range(len(table) - 1):
            value = jnp.where(t == k, table[k], value)
        return value

    def turn(t, carry):
        for k in range(len(steps)):
            pl.when(t == k)(functools.partial(before, k))
        step([[pick(t, [s[i][j] for s in steps]) for j in range(2)] for i in range(2)])
        for k in range(len(steps)):
            pl.when(t == k)(functools.partial(after, k))
        return carry

    lax.fori_loop(0, len(steps), turn, 0)
    pair[3].start()
    pair[3].wait_recv()
    for h in range(heads):
        dq = (dqt[0, h] + dqr[h]) * scale
        dq_ref[:, h * width:(h + 1) * width] = dq.T.astype(BF16)
    total = plane_sum(0)
    part_copy(0, 3).wait_recv()
    total = total + red[0, 3].astype(F32)
    for dz in direct:
        part_copy(dz, 3).wait_recv()
        total = total + red[dz, 3].astype(F32)
    for dz in range(1, nz):
        z_copy(dz).wait_recv()
        total = total + zred[dz].astype(F32)
    dk_ref[...] = (total[:rows] * scale).astype(BF16)
    dv_ref[...] = total[rows:].astype(BF16)

    for copy in pair:
        copy.wait_send()
    for dz in range(nz):
        for dp in (1, 2, 3):
            if dz in folded:
                fold_copy(dz, dp).wait_send()
            else:
                part_copy(dz, dp).wait_send()
        for dp in (1, 2):
            plane_copy(dz, dp).wait_send()
            if dz > 0 and dz not in climb:
                relay_copy(dz, dp).wait_send()
        if dz > 0:
            column_copy(dz).wait_send()
            z_copy(dz).wait_send()
    plane_copy(0, 3).wait_send()
    for dz in climb:
        climb_copy(dz).wait_send()


def write_out(*refs):
    for src, dst in zip(refs[:3], refs[3:]):
        dst[...] = src[...]


def solution(mesh):
    pb_size, ka_size = mesh.shape["pb"], mesh.shape["ka"]

    def body(queries, key_rows, value_rows, forward_out, out_grad, logsumexp, position, segment):
        rows, width = key_rows.shape
        heads = queries.shape[1] // width
        nz, plane = ka_size // 2, pb_size
        both = 2 * rows
        dma, vmem = pltpu.SemaphoreType.DMA, pltpu.VMEM
        space = pl.BlockSpec(memory_space=pltpu.VMEM)
        grads = pl.pallas_call(
            functools.partial(kernel, pb_size, ka_size),
            out_shape=(
                jax.ShapeDtypeStruct(queries.shape, BF16),
                jax.ShapeDtypeStruct(key_rows.shape, BF16),
                jax.ShapeDtypeStruct(key_rows.shape, BF16),
            ),
            in_specs=[pl.BlockSpec(memory_space=pltpu.HBM)] * 5 + [space] * 3,
            out_specs=(space,) * 3,
            scratch_shapes=[
                vmem((nz, plane, both + 16, width), BF16),
                vmem((heads, both, width), BF16),
                vmem((heads, both, width), BF16),
                vmem((heads, rows, width), BF16),
                vmem((2 * heads + 8, rows), F32),
                vmem((2 * heads + 8, rows), F32),
                vmem((both, both), F32),
                vmem((both, heads * both), BF16),
                vmem((both, heads * both), BF16),
                vmem((2, heads, width, rows), F32),
                vmem((heads, width, rows), F32),
                vmem((nz, plane, both, width), BF16),
                vmem((nz, plane, both, width), BF16),
                vmem((nz, plane, both, width), F32),
                vmem((nz, both, width), BF16),
                vmem((nz, both, width), BF16),
                vmem((nz, plane, both, width), BF16),
                dma((3 * heads + 2,)), dma((nz, plane)), dma((nz, plane)),
                dma((nz, 2)), dma((nz, 2)), dma((4,)), dma((4,)),
                dma((nz, plane)), dma((nz, plane)),
                dma((nz,)), dma((nz,)), dma((nz, plane)), dma((nz, plane)),
            ],
            compiler_params=pltpu.CompilerParams(
                collective_id=0, has_side_effects=True, vmem_limit_bytes=48 * 2**20
            ),
        )(*(pltpu.with_memory_space_constraint(x, pltpu.HBM) for x in (
            queries, out_grad, forward_out, key_rows, value_rows, logsumexp,
            position.reshape(1, rows), segment.reshape(1, rows),
        )))
        return pl.pallas_call(
            write_out,
            out_shape=tuple(jax.ShapeDtypeStruct(g.shape, g.dtype) for g in grads),
            in_specs=[space] * 3,
            out_specs=(space,) * 3,
            compiler_params=pltpu.CompilerParams(vmem_limit_bytes=4 * 2**20),
        )(*grads)

    flat = P(("pb", "ka"), None)
    line = P(("pb", "ka"))
    return jax.shard_map(
        body,
        mesh=mesh,
        in_specs=(flat,) * 5 + (P(None, ("pb", "ka")), line, line),
        out_specs=(flat,) * 3,
        check_vma=False,
    )
```

```python
import functools

import jax
import jax.numpy as jnp
from jax import lax
from jax.experimental import pallas as pl
from jax.experimental.pallas import tpu as pltpu
from jax.sharding import PartitionSpec as P

MESH = pl.DeviceIdType.MESH
LOG2E = 1.4426950408889634
HIDDEN = -1e30
NT = (((1,), (1,)), ((), ()))
F32 = jnp.float32
BF16 = jnp.bfloat16


def schedule(nz):
    ranks = [0, nz - 1] + list(range(1, nz - 1))
    order = []
    for r, dz in enumerate(ranks):
        late = (0.0, 0.5, 0.6, 1.1) if r == 0 else (0.0, 1.3, 1.4, {1: 2.65, 2: 1.45}.get(r, 1.5))
        order += [(r + late[dp], dz, dp) for dp in range(4)]
    order.sort()
    blocks = [b[1:] for b in order]
    steps = [blocks[i:i + 2] for i in range(0, len(blocks), 2)]
    when = {b: t for t, step in enumerate(steps) for b in step}
    part = max(1, nz // 4)
    climb = list(range(1, nz - 1))
    direct = ranks[-part:]
    folded = [dz for dz in range(1, part + 1) if dz not in direct]
    return steps, when, climb, direct, folded, ranks


def kernel(
    pb_size, ka_size,
    q_hbm, g_hbm, o_hbm, k_hbm, v_hbm, lse_ref, place_ref, doc_ref,
    dq_ref, dk_ref, dv_ref,
    kv, qs, gs, os, own, sp, bias, pt, st, dqt, dqr,
    part, red, acc, zpart, zred, fold,
    load, kv_send, kv_recv, relay_send, relay_recv, pair_send, pair_recv,
    red_send, red_recv, z_send, z_recv, fold_send, fold_recv,
):
    rows, width = dk_ref.shape
    heads = q_hbm.shape[1] // width
    both = 2 * rows
    scale = width ** (-0.5)
    nz, plane = ka_size // 2, pb_size
    pb, ka = lax.axis_index("pb"), lax.axis_index("ka")
    hi, core = pb // 2, lax.rem(pb, 2)
    z, low = ka // 2, lax.rem(ka, 2)

    def place(dz, dp):
        up, bit = z, 1
        while bit < nz:
            mine, flip = (z // bit) % 2, (dz // bit) % 2
            up = up + flip * (1 - 2 * mine) * bit
            bit *= 2
        far = 1 - hi if dp // 2 else hi
        near = 1 - low if dp % 2 else low
        return {"pb": far * 2 + core, "ka": up * 2 + near}

    partner = {"pb": hi * 2 + 1 - core, "ka": ka}

    def remote(src, dst, send, recv, device):
        return pltpu.make_async_remote_copy(
            src_ref=src, dst_ref=dst, send_sem=send, recv_sem=recv,
            device_id=device, device_id_type=MESH,
        )

    loads = [
        pltpu.make_async_copy(k_hbm, kv.at[0, 0, pl.ds(0, rows)], load.at[0]),
        pltpu.make_async_copy(v_hbm, kv.at[0, 0, pl.ds(rows, rows)], load.at[1]),
    ]
    for src, dst in ((q_hbm, qs), (g_hbm, gs), (o_hbm, os)):
        for h in range(heads):
            loads.append(pltpu.make_async_copy(
                src.at[:, pl.ds(h * width, width)], dst.at[h, pl.ds(0, rows)], load.at[len(loads)]
            ))
    for copy in loads:
        copy.start()

    barrier = pltpu.get_barrier_semaphore()
    steps, when, climb, direct, folded, ranks = schedule(nz)
    last = len(steps) - 1
    peers = [place(dz, 0) for dz in range(1, nz)] + [place(0, dp) for dp in range(1, plane)] + [partner]
    for peer in peers:
        pl.semaphore_signal(barrier, inc=1, device_id=peer, device_id_type=MESH)

    spots = place_ref[...].astype(F32)
    docs = doc_ref[...].astype(F32)
    line = lax.broadcasted_iota(jnp.int32, (16, rows), 0)
    first = jnp.min(spots, axis=1, keepdims=True) * (1.0 / rows)
    meta = jnp.where(line == 0, jnp.broadcast_to(first, (16, rows)), jnp.broadcast_to(docs, (16, rows)))
    kv[0, 0, both:both + 16, :] = meta.astype(BF16)
    own[:heads] = lse_ref[...]
    own[2 * heads:2 * heads + 8] = jnp.where(
        line[:8] == 0, jnp.broadcast_to(spots, (8, rows)), jnp.broadcast_to(docs, (8, rows))
    )
    for copy in loads[:2]:
        copy.wait()
    pl.semaphore_wait(barrier, len(peers))

    def column_copy(dz):
        return remote(kv.at[0, 0], kv.at[dz, 0], kv_send.at[dz, 0], kv_recv.at[dz, 0], place(dz, 0))

    def plane_copy(dz, dp):
        return remote(kv.at[dz, 0], kv.at[dz, dp], kv_send.at[dz, dp], kv_recv.at[dz, dp], place(0, dp))

    def relay_copy(dz, dp):
        piece = pl.ds(0, rows) if dp == 1 else pl.ds(rows, rows + 16)
        return remote(
            kv.at[dz, 3 - dp, piece], kv.at[dz, 3, piece],
            relay_send.at[dz, dp - 1], relay_recv.at[dz, dp - 1], place(0, dp),
        )

    def climb_copy(dz):
        return remote(kv.at[0, 3], kv.at[dz, 3], kv_send.at[dz, 3], kv_recv.at[dz, 3], place(dz, 0))

    def part_copy(dz, dp):
        far = dz if dp == 3 and dz in direct else 0
        return remote(part.at[dz, dp], red.at[dz, dp], red_send.at[dz, dp], red_recv.at[dz, dp], place(far, dp))

    def fold_copy(dz):
        return remote(part.at[dz, 3], fold.at[dz], fold_send.at[dz], fold_recv.at[dz], place(dz, 0))

    def z_copy(dz):
        return remote(zpart.at[dz], zred.at[dz], z_send.at[dz], z_recv.at[dz], place(dz, 0))

    ours, theirs = pl.ds(0, rows), pl.ds(rows, rows)
    pair = [
        remote(src, dst, pair_send.at[i], pair_recv.at[i], partner)
        for i, (src, dst) in enumerate((
            (qs.at[:, ours], qs.at[:, theirs]), (gs.at[:, ours], gs.at[:, theirs]),
            (own, sp), (dqt.at[1], dqr),
        ))
    ]
    for dp in (1, 2):
        plane_copy(0, dp).start()
    for dz in ranks[1:]:
        column_copy(dz).start()
    plane_copy(0, 3).start()
    dqt[...] = jnp.zeros_like(dqt)
    for copy in loads[2:2 + 2 * heads]:
        copy.wait()
    for copy in pair[:2]:
        copy.start()
    for copy in loads[2 + 2 * heads:]:
        copy.wait()
    for h in range(heads):
        product = gs[h, :rows].astype(F32) * os[h].astype(F32)
        own[heads + h:heads + h + 1] = jnp.sum(product.T, axis=0, keepdims=True)
    pair[2].start()

    def spread(dz):
        column_copy(dz).wait_recv()
        for dp in (1, 2):
            plane_copy(dz, dp).start()

    def pass_on(dz):
        for dp in (2, 1):
            plane_copy(dz, 3 - dp).wait_recv()
            if dz not in climb:
                relay_copy(dz, dp).start()

    for copy in pair[:3]:
        copy.wait_recv()

    def stat_row(i):
        return jnp.concatenate([own[i:i + 1, :], sp[i:i + 1, :]], axis=1)

    place_q = stat_row(2 * heads)
    doc_q = stat_row(2 * heads + 1)

    def key_side(dz, dp):
        meta = kv[dz, dp, both:both + 16, :].astype(F32)
        base = jnp.broadcast_to(meta[0:1, :], (rows, rows))
        doc = jnp.broadcast_to(meta[1:2, :], (rows, rows)).T
        spot = base * float(rows) + lax.broadcasted_iota(jnp.int32, (rows, rows), 0).astype(F32)
        return spot, doc

    def step(blocks):
        (za, pa), (zb, pc) = blocks
        for i, (dz, dp) in enumerate(blocks):
            spot, doc = key_side(dz, dp)
            for c in range(2):
                lanes = slice(c * rows, (c + 1) * rows)
                seen = (spot <= place_q[:, lanes]) & (doc == doc_q[:, lanes])
                bias[i * rows:(i + 1) * rows, lanes] = jnp.where(seen, 0.0, HIDDEN)
        kb = jnp.concatenate([kv[za, pa, :rows, :], kv[zb, pc, :rows, :]], axis=0)
        vb = jnp.concatenate([kv[za, pa, rows:both, :], kv[zb, pc, rows:both, :]], axis=0)
        kt = kb.T
        for h in range(heads):
            s = lax.dot_general(kb, qs[h], NT, preferred_element_type=F32)
            d = lax.dot_general(vb, gs[h], NT, preferred_element_type=F32)
            w = jnp.exp2(s * (scale * LOG2E) + (bias[...] - stat_row(h) * LOG2E))
            pt[:, h * both:(h + 1) * both] = w.astype(BF16)
            st[:, h * both:(h + 1) * both] = (w * (d - stat_row(heads + h))).astype(BF16)
        dv = jnp.dot(pt[...], gs[...].reshape(heads * both, width), preferred_element_type=F32)
        dk = jnp.dot(st[...], qs[...].reshape(heads * both, width), preferred_element_type=F32)
        for i, (dz, dp) in enumerate(blocks):
            piece = slice(i * rows, (i + 1) * rows)
            acc[dz, dp, :rows] = dk[piece]
            acc[dz, dp, rows:] = dv[piece]
            part[dz, dp, :rows] = dk[piece].astype(BF16)
            part[dz, dp, rows:] = dv[piece].astype(BF16)
        for h in range(heads):
            dq = jnp.dot(kt, st[:, h * both:(h + 1) * both], preferred_element_type=F32)
            dqt[0, h] += dq[:, :rows]
            dqt[1, h] += dq[:, rows:]

    def plane_sum(dz):
        total = acc[dz, 0]
        for dp in (1, 2) if dz == 0 or dz in folded or dz in direct else (1, 2, 3):
            part_copy(dz, dp).wait_recv()
            total = total + red[dz, dp].astype(F32)
        return total

    def send_sum(dz):
        zpart[dz] = plane_sum(dz).astype(BF16)
        z_copy(dz).start()

    def corner():
        total = acc[0, 3]
        for dz in folded:
            fold_copy(dz).wait_recv()
            total = total + fold[dz].astype(F32)
        part[0, 3] = total.astype(BF16)
        part_copy(0, 3).start()

    def before(t):
        if t == when[0, 3]:
            plane_copy(0, 3).wait_recv()
            for dz in climb:
                climb_copy(dz).start()
        for r, dz in enumerate(ranks):
            if r and max(0, when[dz, 0] - {1: 0, 2: 0}.get(r, 1)) == t:
                spread(dz)
        for b in steps[t]:
            if b[0] == 0 and b[1] in (1, 2):
                plane_copy(*b).wait_recv()
        for dz in ranks[1:]:
            if min(when[dz, 1], when[dz, 2]) == t:
                pass_on(dz)
        for b in steps[t]:
            if b[0] in climb and b[1] == 3:
                climb_copy(b[0]).wait_recv()
            elif b[0] > 0 and b[1] == 3:
                for dp in (1, 2):
                    relay_copy(b[0], dp).wait_recv()

    def after(t):
        for b in reversed([b for s in steps for b in s]):
            if b[1] and b != (0, 3) and min(last, when[b] + {0: 3}.get(b[0], 0)) == t:
                if b[1] == 3 and b[0] in folded:
                    fold_copy(b[0]).start()
                else:
                    part_copy(*b).start()
        if t == last:
            corner()
        for dz in range(1, nz):
            if max(when[dz, dp] for dp in range(3 if dz in direct else 4)) + 2 == t:
                send_sum(dz)

    def pick(t, table):
        value = jnp.int32(table[-1])
        for k in range(len(table) - 1):
            value = jnp.where(t == k, table[k], value)
        return value

    def turn(t, carry):
        for k in range(len(steps)):
            pl.when(t == k)(functools.partial(before, k))
        step([[pick(t, [s[i][j] for s in steps]) for j in range(2)] for i in range(2)])
        for k in range(len(steps)):
            pl.when(t == k)(functools.partial(after, k))
        return carry

    lax.fori_loop(0, len(steps), turn, 0)
    pair[3].start()
    for dz in range(1, nz):
        if max(when[dz, dp] for dp in range(3 if dz in direct else 4)) + 2 > last:
            send_sum(dz)
    pair[3].wait_recv()
    for h in range(heads):
        dq = (dqt[0, h] + dqr[h]) * scale
        dq_ref[:, h * width:(h + 1) * width] = dq.T.astype(BF16)
    total = plane_sum(0)
    part_copy(0, 3).wait_recv()
    total = total + red[0, 3].astype(F32)
    for dz in direct:
        part_copy(dz, 3).wait_recv()
        total = total + red[dz, 3].astype(F32)
    for dz in range(1, nz):
        z_copy(dz).wait_recv()
        total = total + zred[dz].astype(F32)
    dk_ref[...] = (total[:rows] * scale).astype(BF16)
    dv_ref[...] = total[rows:].astype(BF16)

    for copy in pair:
        copy.wait_send()
    for dz in range(nz):
        for dp in (1, 2):
            part_copy(dz, dp).wait_send()
            plane_copy(dz, dp).wait_send()
            if dz > 0 and dz not in climb:
                relay_copy(dz, dp).wait_send()
        if dz in folded:
            fold_copy(dz).wait_send()
        else:
            part_copy(dz, 3).wait_send()
        if dz > 0:
            column_copy(dz).wait_send()
            z_copy(dz).wait_send()
    plane_copy(0, 3).wait_send()
    for dz in climb:
        climb_copy(dz).wait_send()


def write_out(*refs):
    for src, dst in zip(refs[:3], refs[3:]):
        dst[...] = src[...]


def solution(mesh):
    pb_size, ka_size = mesh.shape["pb"], mesh.shape["ka"]

    def body(queries, key_rows, value_rows, forward_out, out_grad, logsumexp, position, segment):
        rows, width = key_rows.shape
        heads = queries.shape[1] // width
        nz, plane = ka_size // 2, pb_size
        both = 2 * rows
        dma, vmem = pltpu.SemaphoreType.DMA, pltpu.VMEM
        space = pl.BlockSpec(memory_space=pltpu.VMEM)
        grads = pl.pallas_call(
            functools.partial(kernel, pb_size, ka_size),
            out_shape=(
                jax.ShapeDtypeStruct(queries.shape, BF16),
                jax.ShapeDtypeStruct(key_rows.shape, BF16),
                jax.ShapeDtypeStruct(key_rows.shape, BF16),
            ),
            in_specs=[pl.BlockSpec(memory_space=pltpu.HBM)] * 5 + [space] * 3,
            out_specs=(space,) * 3,
            scratch_shapes=[
                vmem((nz, plane, both + 16, width), BF16),
                vmem((heads, both, width), BF16),
                vmem((heads, both, width), BF16),
                vmem((heads, rows, width), BF16),
                vmem((2 * heads + 8, rows), F32),
                vmem((2 * heads + 8, rows), F32),
                vmem((both, both), F32),
                vmem((both, heads * both), BF16),
                vmem((both, heads * both), BF16),
                vmem((2, heads, width, rows), F32),
                vmem((heads, width, rows), F32),
                vmem((nz, plane, both, width), BF16),
                vmem((nz, plane, both, width), BF16),
                vmem((nz, plane, both, width), F32),
                vmem((nz, both, width), BF16),
                vmem((nz, both, width), BF16),
                vmem((nz, both, width), BF16),
                dma((3 * heads + 2,)), dma((nz, plane)), dma((nz, plane)),
                dma((nz, 2)), dma((nz, 2)), dma((4,)), dma((4,)),
                dma((nz, plane)), dma((nz, plane)),
                dma((nz,)), dma((nz,)), dma((nz,)), dma((nz,)),
            ],
            compiler_params=pltpu.CompilerParams(
                collective_id=0, has_side_effects=True, vmem_limit_bytes=48 * 2**20
            ),
        )(*(pltpu.with_memory_space_constraint(x, pltpu.HBM) for x in (
            queries, out_grad, forward_out, key_rows, value_rows, logsumexp,
            position.reshape(1, rows), segment.reshape(1, rows),
        )))
        return pl.pallas_call(
            write_out,
            out_shape=tuple(jax.ShapeDtypeStruct(g.shape, g.dtype) for g in grads),
            in_specs=[space] * 3,
            out_specs=(space,) * 3,
            compiler_params=pltpu.CompilerParams(vmem_limit_bytes=4 * 2**20),
        )(*grads)

    flat = P(("pb", "ka"), None)
    line = P(("pb", "ka"))
    return jax.shard_map(
        body,
        mesh=mesh,
        in_specs=(flat,) * 5 + (P(None, ("pb", "ka")), line, line),
        out_specs=(flat,) * 3,
        check_vma=False,
    )
```
